32 devices in a mesh: rep: 4 (over x, core), shard: 8 (over z, y).
Axes of the slice: x: 2, y: 2, z: 4, core: 2. Of those that a mesh axis runs over, the one named last changes fastest.
Arguments:
- dense_out: bfloat16 [4096, 128], P(('rep', 'shard')), may hold values from -0.75 to 0.75
- pooled: bfloat16 [4096, 26, 128], P(('rep', 'shard')), may hold values from -0.75 to 0.75
- top_weight: bfloat16 [479, 1024], replicated, may hold values from -0.25 to 0.25
- top_cotangent: bfloat16 [4096, 1024], P(('rep', 'shard')), may hold values from -3 to 3
- indices: int32 [4096, 26, 2], P(('rep', 'shard')), may hold values from 0 to 2047, as said below
Outputs:
- dense_grad: bfloat16 [4096, 128], P(('rep', 'shard'))
- top_grad: float32 [479, 1024], replicated
- bias_grad: float32 [1024], replicated
- table_grad: float32 [26, 2048, 128], P(None, 'shard')
The draws below stay inside these ranges and needn't reach their ends.
Inputs may be any that keep to these rules, and one draw needn't show every extreme that they name: `indices`: rows r with r // 256 = s are held by shard s. For every device's 128 samples and every table, at most 16 of the device's lookups fall in any one block of 64 rows starting at a multiple of 64, and some such block holds exactly 16.
All inputs are finite; a program needn't handle non-finite values.
Results may differ from the reference program's by a relative error of at most 0.008.
Values may be sent and summed in bfloat16 or wider, within the bound.
A program may use at most 128 MiB of HBM per device.

```python
import jax
import jax.numpy as jnp
import numpy as np
from jax import lax

E = 128
F = 26
H = 1024
B_DEV = 128
L = 2
R_SHARD = 256
IN = 479
BATCH = 4096
ROWS = 2048
N_REP = 4
N_SHARD = 8


def draw_indices(key, part):
    devices_all = N_REP * N_SHARD
    blocks = N_SHARD * N_REP
    per_block = 2 * B_DEV * L // blocks
    lookups = B_DEV * L
    row_span = R_SHARD // N_REP
    places = blocks * per_block

    def draw_bag(subkey):
        key_full, key_order, key_offset, key_shuffle = jax.random.split(subkey, 4)
        full_block = jax.random.randint(key_full, (), 0, blocks, dtype=jnp.int32)
        place_ids = jnp.arange(places, dtype=jnp.int32)
        ranking = jax.random.permutation(key_order, places).astype(jnp.int32)
        scores = jnp.where(place_ids // per_block == full_block, place_ids - places, ranking)
        chosen = jnp.argsort(scores, stable=True)[:lookups].astype(jnp.int32)
        offsets = jax.random.randint(key_offset, (lookups,), 0, row_span, dtype=jnp.int32)
        rows_drawn = chosen // per_block * row_span + offsets
        shuffle = jax.random.permutation(key_shuffle, lookups)
        return rows_drawn[shuffle].reshape(B_DEV, L)
    subkeys = jax.random.split(key, devices_all * F)
    drawn_rows = jax.vmap(draw_bag)(subkeys).reshape(devices_all, F, B_DEV, L)
    return jnp.transpose(drawn_rows, (0, 2, 1, 3)).reshape(devices_all * B_DEV, F, L).astype(jnp.int32)


def steps_of(rng, extent, shards, smallest, high):
    factor_of, own = 1.0, jax.random.fold_in(rng, 6)
    for position, blocks in shards:
        draws = jnp.exp(jax.random.uniform(jax.random.fold_in(own, position), (blocks,), jnp.float32, smallest / len(shards), high / len(shards)))
        factor_of = factor_of * jnp.repeat(draws, extent[position] // blocks).reshape([-1 if axis == position else 1 for axis in range(len(extent))])
    return factor_of


def bell_draw(rng, shape, deviation, bound, pieces=(), held_as=jnp.bfloat16):
    factor_of = steps_of(rng, shape, pieces, -0.22, 0.18) if pieces else 1.0
    array = jax.random.normal(rng, shape, jnp.float32) * deviation * factor_of
    return jnp.minimum(jnp.maximum(array, -bound), bound).astype(held_as)


def setup_inputs(seed: int = 0) -> dict:
    keys = jax.random.split(jax.random.key(seed), 6)
    return {
        "dense_out": bell_draw(keys[0], (BATCH, E), 0.125, 0.75, ((0, 32),)),
        "pooled": bell_draw(keys[1], (BATCH, F, E), 0.125, 0.75, ((0, 32),)),
        "top_weight": bell_draw(keys[2], (IN, H), IN ** -0.5, 0.25),
        "top_cotangent": bell_draw(keys[3], (BATCH, H), 0.5, 3.0, ((0, 32),)),
        "indices": draw_indices(jax.random.fold_in(keys[5], 71), 0),
    }


highest = lax.Precision.HIGHEST


def reference(dense_out, pooled, top_weight, top_cotangent, indices):
    vectors = F + 1
    lower_i, lower_j = np.tril_indices(vectors, -1)
    blocks = BATCH // B_DEV
    table_index = jnp.arange(F, dtype=jnp.int32)

    def block_step(totals, inputs):
        top_acc, bias_acc, table_acc = totals
        dense_block, pooled_block, cot_block, index_block = inputs
        stacked = jnp.concatenate([dense_block[:, None, :], pooled_block], axis=1).astype(jnp.float32)
        gram_matrix = jnp.einsum("bie,bje->bij", stacked, stacked, precision=highest)
        pair_values = gram_matrix[:, lower_i, lower_j].astype(jnp.bfloat16)
        joined = jnp.concatenate([dense_block, pair_values], axis=1)
        grad_in = jnp.dot(cot_block, top_weight.T, preferred_element_type=jnp.float32)
        top_acc = top_acc + jnp.dot(joined.T, cot_block, preferred_element_type=jnp.float32)
        bias_acc = bias_acc + jnp.sum(cot_block.astype(jnp.float32), axis=0)
        pair_grad = grad_in[:, E:]
        mirror = jnp.zeros((pair_grad.shape[0], vectors, vectors), jnp.float32)
        mirror = mirror.at[:, lower_i, lower_j].set(pair_grad)
        mirror = mirror.at[:, lower_j, lower_i].set(pair_grad)
        vec_grad = jnp.einsum("bij,bje->bie", mirror, stacked, precision=highest)
        dense_grad = (grad_in[:, :E] + vec_grad[:, 0]).astype(jnp.bfloat16)
        pooled_grad = vec_grad[:, 1:].astype(jnp.bfloat16)
        updates = jnp.broadcast_to(pooled_grad.astype(jnp.float32)[:, :, None, :], (B_DEV, F, L, E))
        table_acc = table_acc.at[table_index[None, :, None], index_block].add(updates)
        return (top_acc, bias_acc, table_acc), dense_grad

    start = (jnp.zeros((IN, H), jnp.float32), jnp.zeros((H,), jnp.float32), jnp.zeros((F, ROWS, E), jnp.float32))
    inputs = (dense_out.reshape(blocks, B_DEV, E), pooled.reshape(blocks, B_DEV, F, E), top_cotangent.reshape(blocks, B_DEV, H), indices.reshape(blocks, B_DEV, F, L))
    totals, dense_parts = lax.scan(block_step, start, inputs)
    top_grad, bias_grad, table_grad = totals
    return dense_parts.reshape(BATCH, E), top_grad, bias_grad, table_grad
```

```python
import functools

import jax
import jax.numpy as jnp
from jax import lax
from jax.experimental import pallas as pl
from jax.experimental.pallas import tpu as pltpu
from jax.sharding import PartitionSpec as P

PAIR = 2
MESH = pl.DeviceIdType.MESH
VMEM = pl.BlockSpec(memory_space=pltpu.VMEM)
f32, bf16 = jnp.float32, jnp.bfloat16


def cdiv(a, b):
    return -(-a // b)


def local_kernel(nv, group, chunk, dense, pooled, weight, cot, dense_grad, rows_out, top_out, v, gram, mir, joined, grads, vg):
    emb, samples = v.shape[1], v.shape[2]
    features = weight.shape[0]
    v[0] = dense[...].astype(f32).T

    def load(t, _):
        v[t + 1] = pooled[t].astype(f32).T
        return 0

    lax.fori_loop(0, nv - 1, load, 0)
    grads[pl.ds(0, features), :] = lax.dot_general(
        weight[...], cot[...], (((1,), (1,)), ((), ())), preferred_element_type=f32
    )
    for start in range(0, nv, group):
        js = range(start, min(start + group, nv))

        def one(i, _, js=js):
            for j in js:
                gram[i, pl.ds(j, 1), :] = jnp.sum(v[i] * v[j], axis=0, keepdims=True)
            return 0

        lax.fori_loop(start + 1, nv, one, 0)
    joined[...] = jnp.zeros_like(joined)
    joined[pl.ds(0, emb), :] = v[0]
    mir[...] = jnp.zeros_like(mir)
    for i in range(1, nv):
        base = emb + i * (i - 1) // 2
        joined[pl.ds(base, i), :] = gram[i, pl.ds(0, i), :]
        mir[i, pl.ds(0, i), :] = grads[pl.ds(base, i), :]
        for j in range(i):
            mir[j, pl.ds(i, 1), :] = grads[pl.ds(base + j, 1), :]
    joined[pl.ds(features, 1), :] = jnp.ones((1, samples), f32)
    groups, width = top_out.shape[0], top_out.shape[2]
    left = joined[...].astype(bf16)
    for r in range(groups):
        top_out[r] = jnp.dot(
            left, cot[:, pl.ds(r * width, width)], preferred_element_type=f32
        ).astype(bf16)

    def part(c, _):
        where = pl.ds(pl.multiple_of(c * chunk, chunk), chunk)
        for start in range(0, nv, group):
            items = range(start, min(start + group, nv))

            def add(j, accs):
                vj = v[j, where, :]
                return tuple(a + vj * mir[j, pl.ds(i, 1), :] for a, i in zip(accs, items))

            accs = lax.fori_loop(
                0, nv, add, tuple(jnp.zeros((chunk, samples), f32) for _ in items)
            )
            for a, i in zip(accs, items):
                vg[i, where, :] = a
        return 0

    lax.fori_loop(0, emb // chunk, part, 0)
    dense_grad[...] = (grads[pl.ds(0, emb), :] + vg[0]).T.astype(bf16)

    def store(t, _):
        rows_out[t] = vg[t + 1].T.astype(bf16)
        return 0

    lax.fori_loop(0, nv - 1, store, 0)
    for t in range(nv - 1, rows_out.shape[0]):
        rows_out[t] = jnp.zeros_like(rows_out[t])


def comm_kernel(
    R, S, lookups, rows_in, keys_in, top_in, tab_out, top_out,
    rows, keys, part, prcv, own, fin, trcv, tsum, tred, tfin, tgat,
    s_rows, r_rows, s_keys, r_keys, s_top, r_top, s_yrow, r_yrow, s_ykey, r_ykey,
    s_part, r_part, s_fin, r_fin, s_t2, r_t2, s_t3, r_t3, s_t4, r_t4, l_sem,
):
    q, s = lax.axis_index("rep"), lax.axis_index("shard")
    Z = S // PAIR
    y, z = s % PAIR, s // PAIR
    mate = z * PAIR + (1 - y)
    T, span = part.shape[1], part.shape[2]
    B = rows.shape[3]
    chunk_rows = tgat.shape[1]

    def copy(src, dst, ssem, rsem, rep, shard):
        return pltpu.make_async_remote_copy(
            src_ref=src, dst_ref=dst, send_sem=ssem, recv_sem=rsem,
            device_id=(rep, shard), device_id_type=MESH,
        )

    barrier = pltpu.get_barrier_semaphore()
    for k in range(1, R):
        pl.semaphore_signal(barrier, inc=1, device_id=((q + k) % R, s), device_id_type=MESH)

    def greet(k, _):
        pl.semaphore_signal(barrier, inc=1, device_id=(q, (s + k) % S), device_id_type=MESH)
        return 0

    lax.fori_loop(1, S, greet, 0)
    pl.semaphore_wait(barrier, R - 1 + S - 1)

    def rep_copies(k):
        to = (q + k) % R
        return (
            copy(rows_in.at[to], rows.at[y, q], s_rows.at[k - 1], r_rows.at[k - 1], to, s),
            copy(keys_in.at[to], keys.at[y, q], s_keys.at[k - 1], r_keys.at[k - 1], to, s),
        )

    def top_copy(k):
        to = (q + k) % R
        return copy(top_in.at[to], trcv.at[k - 1], s_top.at[k - 1], r_top.at[k - 1], to, s)

    for k in range(1, R):
        for c in rep_copies(k):
            c.start()
    mine = pltpu.make_async_copy(rows_in.at[q], rows.at[y, q], l_sem.at[0])
    mine.start()
    mine_keys = pltpu.make_async_copy(keys_in.at[q], keys.at[y, q], l_sem.at[1])
    mine_keys.start()
    for k in range(1, R):
        top_copy(k).start()
    mine.wait()
    mine_keys.wait()

    def pair_copies(k):
        r = (q + R - k) % R
        return (
            copy(rows.at[y, r], rows.at[y, r], s_yrow.at[k], r_yrow.at[k], q, mate),
            copy(keys.at[y, r], keys.at[y, r], s_ykey.at[k], r_ykey.at[k], q, mate),
        )

    for c in pair_copies(0):
        c.start()
    for k in range(1, R):
        for c in rep_copies(k):
            c.wait_recv()
        for c in pair_copies(k):
            c.start()

    for k in range(1, R):
        top_copy(k).wait_recv()
    total = top_in[q].astype(f32)
    for k in range(1, R):
        total = total + trcv[k - 1].astype(f32)
    tsum[...] = total.astype(bf16).reshape(tsum.shape)

    def t2_copy(k):
        to = (s + k) % S
        return copy(tsum.at[to], tred.at[k - 1], s_t2.at[k - 1], r_t2.at[k - 1], q, to)

    def t3_copy(k):
        to = (s + k) % S
        return copy(tfin, tgat.at[s], s_t3.at[k - 1], r_t3.at[k - 1], q, to)

    def each(n, f):
        def step(k, _):
            f(k)
            return 0

        lax.fori_loop(1, n, step, 0)

    each(S, lambda k: t2_copy(k).start())

    for k in range(R):
        for c in pair_copies(k):
            c.wait_recv()

    levels = lax.broadcasted_iota(jnp.int32, (span, B), 0)

    def partial_of(t, shard):
        acc = jnp.zeros((span, rows.shape[4]), f32)
        for side in range(PAIR):
            for r in range(R):
                hits = None
                for l in range(lookups):
                    key = keys[side, r, pl.ds(t * lookups + l, 1), :] - shard * span
                    hit = jnp.where(levels == key, 1.0, 0.0)
                    hits = hit if hits is None else hits + hit
                acc = acc + jnp.dot(hits.astype(bf16), rows[side, r, t], preferred_element_type=f32)
        return acc

    def part_copy(k):
        to = ((z + k) % Z) * PAIR + y
        return copy(part.at[k - 1], prcv.at[k - 1], s_part.at[k - 1], r_part.at[k - 1], q, to)

    def send_part(k):
        to = ((z + k) % Z) * PAIR + y

        def table(t, _):
            part[k - 1, t] = partial_of(t, to).astype(bf16)
            return 0

        lax.fori_loop(0, T, table, 0)
        part_copy(k).start()

    each(Z, send_part)

    each(S, lambda k: t2_copy(k).wait_recv())
    tfin[...] = lax.fori_loop(
        1, S, lambda k, a: a + tred[k - 1].astype(f32), tsum[s].astype(f32)
    ).astype(bf16)
    each(S, lambda k: t3_copy(k).start())

    def own_table(t, _):
        own[t] = partial_of(t, s)
        return 0

    lax.fori_loop(0, T, own_table, 0)
    tgat[s] = tfin[...]
    each(S, lambda k: t3_copy(k).wait_recv())

    def t4_copy(k):
        to = (q + k) % R
        return copy(tgat, top_out.at[q], s_t4.at[k - 1], r_t4.at[k - 1], to, s)

    def fin_copy(k):
        to = (q + k) % R
        return copy(fin, tab_out.at[q], s_fin.at[k - 1], r_fin.at[k - 1], to, s)

    for k in range(1, R):
        t4_copy(k).start()
    each(Z, lambda k: part_copy(k).wait_recv())

    def finish(t, _):
        fin[t] = lax.fori_loop(
            1, Z, lambda k, a: a + prcv[k - 1, t].astype(f32), own[t]
        ).astype(bf16)
        return 0

    lax.fori_loop(0, T, finish, 0)
    for k in range(1, R):
        fin_copy(k).start()
    top_out[q] = tgat[...]
    tab_out[q] = fin[...]
    for k in range(1, R):
        for c in rep_copies(k):
            c.wait_send()
        top_copy(k).wait_send()
    for k in range(R):
        for c in pair_copies(k):
            c.wait_send()
    each(S, lambda k: t2_copy(k).wait_send())
    each(S, lambda k: t3_copy(k).wait_send())
    each(Z, lambda k: part_copy(k).wait_send())
    for k in range(1, R):
        t4_copy(k).wait()
        fin_copy(k).wait()


def on_device(span, R, S, dense_out, pooled, top_weight, top_cotangent, indices):
    samples, emb = dense_out.shape
    tables, lookups = pooled.shape[1], indices.shape[2]
    nv = tables + 1
    features, hidden = top_weight.shape
    T = cdiv(tables, R)
    chunk_rows = cdiv(features + 1, 16 * S) * 16
    height = chunk_rows * S
    width = hidden // R
    pad_v = cdiv(nv, 8) * 8
    dense_grad, rows, top = pl.pallas_call(
        functools.partial(local_kernel, nv, 9, 32),
        out_shape=(
            jax.ShapeDtypeStruct((samples, emb), bf16),
            jax.ShapeDtypeStruct((R * T, samples, emb), bf16),
            jax.ShapeDtypeStruct((R, height, width), bf16),
        ),
        in_specs=[VMEM] * 4,
        out_specs=(VMEM,) * 3,
        scratch_shapes=[
            pltpu.VMEM((nv, emb, samples), f32),
            pltpu.VMEM((nv, pad_v, samples), f32),
            pltpu.VMEM((nv, pad_v, samples), f32),
            pltpu.VMEM((height, samples), f32),
            pltpu.VMEM((cdiv(features, 8) * 8, samples), f32),
            pltpu.VMEM((nv, emb, samples), f32),
        ],
        compiler_params=pltpu.CompilerParams(vmem_limit_bytes=48 << 20),
        name="local_math",
    )(dense_out, jnp.transpose(pooled, (1, 0, 2)), top_weight, top_cotangent)

    keys = jnp.transpose(indices, (1, 2, 0))
    keys = jnp.pad(keys, ((0, R * T - tables), (0, 0), (0, 0)), constant_values=-1)
    keys = keys.reshape(R, T * lookups, samples)
    key_rows = cdiv(T * lookups, 8) * 8
    keys = jnp.pad(keys, ((0, 0), (0, key_rows - T * lookups), (0, 0)), constant_values=-1)

    Z = S // PAIR
    dma = pltpu.SemaphoreType.DMA
    table_all, top_all = pl.pallas_call(
        functools.partial(comm_kernel, R, S, lookups),
        out_shape=(
            jax.ShapeDtypeStruct((R, T, span, emb), bf16),
            jax.ShapeDtypeStruct((R, S, chunk_rows, width), bf16),
        ),
        in_specs=[VMEM] * 3,
        out_specs=(VMEM,) * 2,
        scratch_shapes=[
            pltpu.VMEM((PAIR, R, T, samples, emb), bf16),
            pltpu.VMEM((PAIR, R, key_rows, samples), jnp.int32),
            pltpu.VMEM((Z - 1, T, span, emb), bf16),
            pltpu.VMEM((Z - 1, T, span, emb), bf16),
            pltpu.VMEM((T, span, emb), f32),
            pltpu.VMEM((T, span, emb), bf16),
            pltpu.VMEM((R - 1, S, chunk_rows, width), bf16),
            pltpu.VMEM((S, chunk_rows, width), bf16),
            pltpu.VMEM((S - 1, chunk_rows, width), bf16),
            pltpu.VMEM((chunk_rows, width), bf16),
            pltpu.VMEM((S, chunk_rows, width), bf16),
            dma((R - 1,)), dma((R - 1,)), dma((R - 1,)), dma((R - 1,)), dma((R - 1,)), dma((R - 1,)),
            dma((R,)), dma((R,)), dma((R,)), dma((R,)),
            dma((Z - 1,)), dma((Z - 1,)), dma((R - 1,)), dma((R - 1,)),
            dma((S - 1,)), dma((S - 1,)), dma((S - 1,)), dma((S - 1,)),
            dma((R - 1,)), dma((R - 1,)), dma((2,)),
        ],
        compiler_params=pltpu.CompilerParams(
            collective_id=0, has_side_effects=True, vmem_limit_bytes=60 << 20
        ),
        name="exchange",
    )(rows.reshape(R, T, samples, emb), keys, top.reshape(R, S, chunk_rows, width))
    table_grad = table_all.reshape(R * T, span, emb)[:tables].astype(f32)
    whole = jnp.transpose(top_all.reshape(R, height, width), (1, 0, 2)).reshape(height, hidden)
    top_grad = whole[:features].astype(f32)
    bias_grad = whole[features].astype(f32)
    return dense_grad, top_grad, bias_grad, table_grad


ROWS_PER_SHARD = 256


def solution(mesh):
    return jax.shard_map(
        functools.partial(on_device, ROWS_PER_SHARD, mesh.shape["rep"], mesh.shape["shard"]),
        mesh=mesh,
        in_specs=(
            P(("rep", "shard"), None),
            P(("rep", "shard"), None, None),
            P(),
            P(("rep", "shard"), None),
            P(("rep", "shard"), None, None),
        ),
        out_specs=(P(("rep", "shard"), None), P(), P(), P(None, "shard", None)),
        check_vma=False,
    )
```

```python
import functools

import jax
import jax.numpy as jnp
from jax import lax
from jax.experimental import pallas as pl
from jax.experimental.pallas import tpu as pltpu
from jax.sharding import PartitionSpec as P

PAIR = 2
CORES = 2
MESH = pl.DeviceIdType.MESH
VMEM = pl.BlockSpec(memory_space=pltpu.VMEM)
f32, bf16 = jnp.float32, jnp.bfloat16


def cdiv(a, b):
    return -(-a // b)


def local_kernel(nv, group, chunk, dense, pooled, weight, cot, dense_grad, rows_out, top_out, v, gram, mir, joined, grads, vg):
    emb, samples = v.shape[1], v.shape[2]
    features = weight.shape[0]
    v[0] = dense[...].astype(f32).T

    def load(t, _):
        v[t + 1] = pooled[t].astype(f32).T
        return 0

    lax.fori_loop(0, nv - 1, load, 0)
    grads[pl.ds(0, features), :] = lax.dot_general(
        weight[...], cot[...], (((1,), (1,)), ((), ())), preferred_element_type=f32
    )
    for start in range(0, nv, group):
        js = range(start, min(start + group, nv))

        def one(i, _, js=js):
            for j in js:
                gram[i, pl.ds(j, 1), :] = jnp.sum(v[i] * v[j], axis=0, keepdims=True)
            return 0

        lax.fori_loop(start + 1, nv, one, 0)
    joined[...] = jnp.zeros_like(joined)
    joined[pl.ds(0, emb), :] = v[0]
    mir[...] = jnp.zeros_like(mir)
    for i in range(1, nv):
        base = emb + i * (i - 1) // 2
        joined[pl.ds(base, i), :] = gram[i, pl.ds(0, i), :]
        mir[i, pl.ds(0, i), :] = grads[pl.ds(base, i), :]
        for j in range(i):
            mir[j, pl.ds(i, 1), :] = grads[pl.ds(base + j, 1), :]
    joined[pl.ds(features, 1), :] = jnp.ones((1, samples), f32)
    groups, width = top_out.shape[0], top_out.shape[2]
    left = joined[...].astype(bf16)
    for r in range(groups):
        top_out[r] = jnp.dot(
            left, cot[:, pl.ds(r * width, width)], preferred_element_type=f32
        ).astype(bf16)

    def part(c, _):
        where = pl.ds(pl.multiple_of(c * chunk, chunk), chunk)
        for start in range(0, nv, group):
            items = range(start, min(start + group, nv))

            def add(j, accs):
                vj = v[j, where, :]
                return tuple(a + vj * mir[j, pl.ds(i, 1), :] for a, i in zip(accs, items))

            accs = lax.fori_loop(
                0, nv, add, tuple(jnp.zeros((chunk, samples), f32) for _ in items)
            )
            for a, i in zip(accs, items):
                vg[i, where, :] = a
        return 0

    lax.fori_loop(0, emb // chunk, part, 0)
    dense_grad[...] = (grads[pl.ds(0, emb), :] + vg[0]).T.astype(bf16)

    def store(t, _):
        rows_out[t] = vg[t + 1].T.astype(bf16)
        return 0

    lax.fori_loop(0, nv - 1, store, 0)
    for t in range(nv - 1, rows_out.shape[0]):
        rows_out[t] = jnp.zeros_like(rows_out[t])


def comm_kernel(
    R, S, lookups, rows_in, keys_in, top_in, tab_out, top_out,
    rows, keys, part, prcv, own, trcv, tsum, tred, tfin,
    s_rows, r_rows, s_keys, r_keys, s_top, r_top, s_yrow, r_yrow, s_ykey, r_ykey,
    s_part, r_part, s_fin, r_fin, s_fwd, r_fwd, s_t2, r_t2, s_t3, r_t3,
    s_t4, r_t4, s_t5, r_t5, l_rows, l_keys,
):
    q, s = lax.axis_index("rep"), lax.axis_index("shard")
    Z, X = S // PAIR, R // CORES
    y, z = s % PAIR, s // PAIR
    mate = z * PAIR + (1 - y)
    core = q % CORES
    twin = q - core + (1 - core)
    T, span = own.shape[0], own.shape[1]
    B = rows.shape[3]

    def copy(src, dst, ssem, rsem, rep, shard):
        return pltpu.make_async_remote_copy(
            src_ref=src, dst_ref=dst, send_sem=ssem, recv_sem=rsem,
            device_id=(rep, shard), device_id_type=MESH,
        )

    def each(start, stop, f):
        def step(k, _):
            f(k)
            return 0

        lax.fori_loop(start, stop, step, 0)

    barrier = pltpu.get_barrier_semaphore()
    for k in range(1, R):
        pl.semaphore_signal(barrier, inc=1, device_id=((q + k) % R, s), device_id_type=MESH)
    each(1, S, lambda k: pl.semaphore_signal(
        barrier, inc=1, device_id=(q, (s + k) % S), device_id_type=MESH))
    pl.semaphore_wait(barrier, R - 1 + S - 1)

    def row_copy(t, k):
        to = (q + k) % R
        return copy(rows_in.at[to, t], rows.at[y, t, q], s_rows.at[t, k - 1], r_rows.at[t, k - 1], to, s)

    def own_row_copy(t):
        return pltpu.make_async_copy(rows_in.at[q, t], rows.at[y, t, q], l_rows.at[t])

    def key_copy(k):
        to = (q + k) % R
        return copy(keys_in.at[to], keys.at[y, q], s_keys.at[k - 1], r_keys.at[k - 1], to, s)

    def top_copy(k):
        to = (q + k) % R
        return copy(top_in.at[to], trcv.at[k - 1], s_top.at[k - 1], r_top.at[k - 1], to, s)

    own_keys = pltpu.make_async_copy(keys_in.at[q], keys.at[y, q], l_keys)
    own_keys.start()
    for k in range(1, R):
        key_copy(k).start()

    def send_rows(t):
        own_row_copy(t).start()
        for k in range(1, R):
            row_copy(t, k).start()

    each(0, T, send_rows)
    for k in range(1, R):
        top_copy(k).start()

    def pair_copy(t):
        return copy(rows.at[y, t], rows.at[y, t], s_yrow.at[t], r_yrow.at[t], q, mate)

    def pair_keys():
        return copy(keys.at[y], keys.at[y], s_ykey, r_ykey, q, mate)

    def stage_b(t):
        for k in range(1, R):
            row_copy(t, k).wait_recv()
        own_row_copy(t).wait()
        pair_copy(t).start()

    levels = lax.broadcasted_iota(jnp.int32, (span, B), 0)

    def partial_of(t, shard):
        acc = jnp.zeros((span, rows.shape[4]), f32)
        for side in range(PAIR):
            for r in range(R):
                hits = None
                for l in range(lookups):
                    key = keys[side, r, pl.ds(t * lookups + l, 1), :] - shard * span
                    hit = jnp.where(levels == key, 1.0, 0.0)
                    hits = hit if hits is None else hits + hit
                acc = acc + jnp.dot(hits.astype(bf16), rows[side, t, r], preferred_element_type=f32)
        return acc

    def part_copy(t, k):
        to = ((z + k) % Z) * PAIR + y
        return copy(part.at[t, k - 1], prcv.at[t, k - 1], s_part.at[t, k - 1], r_part.at[t, k - 1], q, to)

    def stage_c(t):
        pair_copy(t).wait_recv()

        def send_part(k):
            part[t, k - 1] = partial_of(t, ((z + k) % Z) * PAIR + y).astype(bf16)
            part_copy(t, k).start()

        each(1, Z, send_part)
        own[t] = partial_of(t, s)

    def fin_copy(t, k):
        to = twin if k == 0 else (q + CORES * k) % R
        return copy(tab_out.at[q, t], tab_out.at[q, t], s_fin.at[t, k], r_fin.at[t, k], to, s)

    def fin_forward(t, k):
        origin = (q + R - CORES * k) % R
        return copy(tab_out.at[origin, t], tab_out.at[origin, t], s_fwd.at[t, k - 1], r_fwd.at[t, k - 1], twin, s)

    def stage_d(t):
        each(1, Z, lambda k: part_copy(t, k).wait_recv())
        tab_out[q, t] = lax.fori_loop(
            1, Z, lambda k, a: a + prcv[t, k - 1].astype(f32), own[t]
        ).astype(bf16)
        for k in reversed(range(X)):
            fin_copy(t, k).start()

    def stage_e(t):
        for k in range(1, X):
            fin_copy(t, k).wait_recv()
            fin_forward(t, k).start()

    def t2_copy(k):
        to = (s + k) % S
        return copy(tsum.at[to], tred.at[k - 1], s_t2.at[k - 1], r_t2.at[k - 1], q, to)

    def t3_copy(k):
        to = (s + k) % S
        return copy(tfin, top_out.at[q, s], s_t3.at[k - 1], r_t3.at[k - 1], q, to)

    def t4_copy(k):
        to = twin if k == 0 else (q + CORES * k) % R
        return copy(top_out.at[q], top_out.at[q], s_t4.at[k], r_t4.at[k], to, s)

    def t5_copy(k):
        origin = (q + R - CORES * k) % R
        return copy(top_out.at[origin], top_out.at[origin], s_t5.at[k - 1], r_t5.at[k - 1], twin, s)

    def top_a():
        total = top_in[q].astype(f32)
        for k in range(1, R):
            top_copy(k).wait_recv()
            total = total + trcv[k - 1].astype(f32)
        tsum[...] = total.astype(bf16)
        each(1, S, lambda k: t2_copy(k).start())

    def top_b():
        each(1, S, lambda k: t2_copy(k).wait_recv())
        tfin[...] = lax.fori_loop(
            1, S, lambda k, a: a + tred[k - 1].astype(f32), tsum[s].astype(f32)
        ).astype(bf16)
        top_out[q, s] = tfin[...]
        each(1, S, lambda k: t3_copy(k).start())

    def top_c():
        each(1, S, lambda k: t3_copy(k).wait_recv())
        for k in reversed(range(X)):
            t4_copy(k).start()

    def top_d():
        for k in range(1, X):
            t4_copy(k).wait_recv()
            t5_copy(k).start()

    own_keys.wait()
    for k in range(1, R):
        key_copy(k).wait_recv()
    pair_keys().start()
    for t in range(min(2, T)):
        stage_b(t)
    pair_keys().wait_recv()

    def step(i, _):
        pl.when(i + 2 < T)(lambda: stage_b(i + 2))
        pl.when(i < T)(lambda: stage_c(i))
        for at, f in ((2, top_a), (4, top_b), (5, top_c), (7, top_d)):
            pl.when(i == at)(f)
        pl.when((i >= 2) & (i < T + 2))(lambda: stage_d(i - 2))
        pl.when((i >= 3) & (i < T + 3))(lambda: stage_e(i - 3))
        return 0

    lax.fori_loop(0, max(T + 3, 8), step, 0)

    def drain(t):
        for k in range(1, R):
            row_copy(t, k).wait_send()
        pair_copy(t).wait_send()
        each(1, Z, lambda k: part_copy(t, k).wait_send())
        fin_copy(t, 0).wait()
        for k in range(1, X):
            fin_copy(t, k).wait_send()
            fin_forward(t, k).wait()

    each(0, T, drain)
    for k in range(1, R):
        key_copy(k).wait_send()
        top_copy(k).wait_send()
    pair_keys().wait_send()
    each(1, S, lambda k: t2_copy(k).wait_send())
    each(1, S, lambda k: t3_copy(k).wait_send())
    t4_copy(0).wait()
    for k in range(1, X):
        t4_copy(k).wait_send()
        t5_copy(k).wait()


def on_device(span, R, S, dense_out, pooled, top_weight, top_cotangent, indices):
    samples, emb = dense_out.shape
    tables, lookups = pooled.shape[1], indices.shape[2]
    nv = tables + 1
    features, hidden = top_weight.shape
    T = cdiv(tables, R)
    chunk_rows = cdiv(features + 1, 16 * S) * 16
    height = chunk_rows * S
    width = hidden // R
    pad_v = cdiv(nv, 8) * 8
    dense_grad, rows, top = pl.pallas_call(
        functools.partial(local_kernel, nv, 9, 32),
        out_shape=(
            jax.ShapeDtypeStruct((samples, emb), bf16),
            jax.ShapeDtypeStruct((R * T, samples, emb), bf16),
            jax.ShapeDtypeStruct((R, height, width), bf16),
        ),
        in_specs=[VMEM] * 4,
        out_specs=(VMEM,) * 3,
        scratch_shapes=[
            pltpu.VMEM((nv, emb, samples), f32),
            pltpu.VMEM((nv, pad_v, samples), f32),
            pltpu.VMEM((nv, pad_v, samples), f32),
            pltpu.VMEM((height, samples), f32),
            pltpu.VMEM((cdiv(features, 8) * 8, samples), f32),
            pltpu.VMEM((nv, emb, samples), f32),
        ],
        compiler_params=pltpu.CompilerParams(vmem_limit_bytes=48 << 20),
        name="local_math",
    )(dense_out, jnp.transpose(pooled, (1, 0, 2)), top_weight, top_cotangent)

    keys = jnp.transpose(indices, (1, 2, 0))
    keys = jnp.pad(keys, ((0, R * T - tables), (0, 0), (0, 0)), constant_values=-1)
    keys = keys.reshape(R, T * lookups, samples)
    key_rows = cdiv(T * lookups, 8) * 8
    keys = jnp.pad(keys, ((0, 0), (0, key_rows - T * lookups), (0, 0)), constant_values=-1)

    Z, X = S // PAIR, R // CORES
    dma = pltpu.SemaphoreType.DMA
    table_all, top_all = pl.pallas_call(
        functools.partial(comm_kernel, R, S, lookups),
        out_shape=(
            jax.ShapeDtypeStruct((R, T, span, emb), bf16),
            jax.ShapeDtypeStruct((R, S, chunk_rows, width), bf16),
        ),
        in_specs=[VMEM] * 3,
        out_specs=(VMEM,) * 2,
        scratch_shapes=[
            pltpu.VMEM((PAIR, T, R, samples, emb), bf16),
            pltpu.VMEM((PAIR, R, key_rows, samples), jnp.int32),
            pltpu.VMEM((T, Z - 1, span, emb), bf16),
            pltpu.VMEM((T, Z - 1, span, emb), bf16),
            pltpu.VMEM((T, span, emb), f32),
            pltpu.VMEM((R - 1, S, chunk_rows, width), bf16),
            pltpu.VMEM((S, chunk_rows, width), bf16),
            pltpu.VMEM((S - 1, chunk_rows, width), bf16),
            pltpu.VMEM((chunk_rows, width), bf16),
            *[dma((T, R - 1))] * 2, *[dma((R - 1,))] * 4, *[dma((T,))] * 2, dma, dma,
            *[dma((T, Z - 1))] * 2, *[dma((T, X))] * 2, *[dma((T, X - 1))] * 2,
            *[dma((S - 1,))] * 4, *[dma((X,))] * 2, *[dma((X - 1,))] * 2, dma((T,)), dma,
        ],
        compiler_params=pltpu.CompilerParams(
            collective_id=0, has_side_effects=True, vmem_limit_bytes=60 << 20
        ),
        name="exchange",
    )(rows.reshape(R, T, samples, emb), keys, top.reshape(R, S, chunk_rows, width))
    table_grad = table_all.reshape(R * T, span, emb)[:tables].astype(f32)
    whole = jnp.transpose(top_all.reshape(R, height, width), (1, 0, 2)).reshape(height, hidden)
    top_grad = whole[:features].astype(f32)
    bias_grad = whole[features].astype(f32)
    return dense_grad, top_grad, bias_grad, table_grad


ROWS_PER_SHARD = 256


def solution(mesh):
    return jax.shard_map(
        functools.partial(on_device, ROWS_PER_SHARD, mesh.shape["rep"], mesh.shape["shard"]),
        mesh=mesh,
        in_specs=(
            P(("rep", "shard"), None),
            P(("rep", "shard"), None, None),
            P(),
            P(("rep", "shard"), None),
            P(("rep", "shard"), None, None),
        ),
        out_specs=(P(("rep", "shard"), None), P(), P(), P(None, "shard", None)),
        check_vma=False,
    )
```

```python
import functools

import jax
import jax.numpy as jnp
from jax import lax
from jax.experimental import pallas as pl
from jax.experimental.pallas import tpu as pltpu
from jax.sharding import PartitionSpec as P

PAIR = 2
CORES = 2
MESH = pl.DeviceIdType.MESH
VMEM = pl.BlockSpec(memory_space=pltpu.VMEM)
f32, bf16 = jnp.float32, jnp.bfloat16


def cdiv(a, b):
    return -(-a // b)


def local_kernel(nv, group, chunk, dense, pooled, weight, cot, dense_grad, rows_out, top_out, v, gram, mir, joined, grads, vg):
    emb, samples = v.shape[1], v.shape[2]
    features = weight.shape[0]
    v[0] = dense[...].astype(f32).T

    def load(t, _):
        v[t + 1] = pooled[t].astype(f32).T
        return 0

    lax.fori_loop(0, nv - 1, load, 0)
    grads[pl.ds(0, features), :] = lax.dot_general(
        weight[...], cot[...], (((1,), (1,)), ((), ())), preferred_element_type=f32
    )
    for start in range(0, nv, group):
        js = range(start, min(start + group, nv))

        def one(i, _, js=js):
            for j in js:
                gram[i, pl.ds(j, 1), :] = jnp.sum(v[i] * v[j], axis=0, keepdims=True)
            return 0

        lax.fori_loop(start + 1, nv, one, 0)
    joined[...] = jnp.zeros_like(joined)
    joined[pl.ds(0, emb), :] = v[0]
    mir[...] = jnp.zeros_like(mir)
    for i in range(1, nv):
        base = emb + i * (i - 1) // 2
        joined[pl.ds(base, i), :] = gram[i, pl.ds(0, i), :]
        mir[i, pl.ds(0, i), :] = grads[pl.ds(base, i), :]
        for j in range(i):
            mir[j, pl.ds(i, 1), :] = grads[pl.ds(base + j, 1), :]
    joined[pl.ds(features, 1), :] = jnp.ones((1, samples), f32)
    groups, width = top_out.shape[0], top_out.shape[2]
    left = joined[...].astype(bf16)
    for r in range(groups):
        top_out[r] = jnp.dot(
            left, cot[:, pl.ds(r * width, width)], preferred_element_type=f32
        ).astype(bf16)

    def part(c, _):
        where = pl.ds(pl.multiple_of(c * chunk, chunk), chunk)
        for start in range(0, nv, group):
            items = range(start, min(start + group, nv))

            def add(j, accs):
                vj = v[j, where, :]
                return tuple(a + vj * mir[j, pl.ds(i, 1), :] for a, i in zip(accs, items))

            accs = lax.fori_loop(
                0, nv, add, tuple(jnp.zeros((chunk, samples), f32) for _ in items)
            )
            for a, i in zip(accs, items):
                vg[i, where, :] = a
        return 0

    lax.fori_loop(0, emb // chunk, part, 0)
    dense_grad[...] = (grads[pl.ds(0, emb), :] + vg[0]).T.astype(bf16)

    def store(t, _):
        rows_out[t] = vg[t + 1].T.astype(bf16)
        return 0

    lax.fori_loop(0, nv - 1, store, 0)
    for t in range(nv - 1, rows_out.shape[0]):
        rows_out[t] = jnp.zeros_like(rows_out[t])


def comm_kernel(
    R, S, lookups, rows_in, keys_in, top_in, tab_out, top_out,
    rows, keys, part, prcv, own, trcv, tsum, tred, tfin,
    s_rows, r_rows, s_keys, r_keys, s_top, r_top, s_yrow, r_yrow, s_ykey, r_ykey,
    s_part, r_part, s_fin, r_fin, s_fwd, r_fwd, s_t2, r_t2, s_t3, r_t3,
    s_t4, r_t4, s_t5, r_t5, l_rows, l_keys,
):
    q, s = lax.axis_index("rep"), lax.axis_index("shard")
    Z, X = S // PAIR, R // CORES
    y, z = s % PAIR, s // PAIR
    mate = z * PAIR + (1 - y)
    core = q % CORES
    twin = q - core + (1 - core)
    T, span = own.shape[0], own.shape[1]
    B = rows.shape[3]

    def copy(src, dst, ssem, rsem, rep, shard):
        return pltpu.make_async_remote_copy(
            src_ref=src, dst_ref=dst, send_sem=ssem, recv_sem=rsem,
            device_id=(rep, shard), device_id_type=MESH,
        )

    def each(start, stop, f):
        def step(k, _):
            f(k)
            return 0

        lax.fori_loop(start, stop, step, 0)

    barrier = pltpu.get_barrier_semaphore()
    for k in range(1, R):
        pl.semaphore_signal(barrier, inc=1, device_id=((q + k) % R, s), device_id_type=MESH)
    each(1, S, lambda k: pl.semaphore_signal(
        barrier, inc=1, device_id=(q, (s + k) % S), device_id_type=MESH))
    pl.semaphore_wait(barrier, R - 1 + S - 1)

    def row_copy(t, k):
        to = (q + k) % R
        return copy(rows_in.at[to, t], rows.at[y, t, q], s_rows.at[t, k - 1], r_rows.at[t, k - 1], to, s)

    def own_row_copy(t):
        return pltpu.make_async_copy(rows_in.at[q, t], rows.at[y, t, q], l_rows.at[t])

    def key_copy(k):
        to = (q + k) % R
        return copy(keys_in.at[to], keys.at[y, q], s_keys.at[k - 1], r_keys.at[k - 1], to, s)

    def top_copy(k):
        to = (q + k) % R
        return copy(top_in.at[to], trcv.at[k - 1], s_top.at[k - 1], r_top.at[k - 1], to, s)

    own_keys = pltpu.make_async_copy(keys_in.at[q], keys.at[y, q], l_keys)
    own_keys.start()
    for k in range(1, R):
        key_copy(k).start()

    def send_rows(t):
        own_row_copy(t).start()
        for k in range(1, R):
            row_copy(t, k).start()

    each(0, T, send_rows)
    for k in range(1, R):
        top_copy(k).start()

    def pair_copy(t):
        return copy(rows.at[y, t], rows.at[y, t], s_yrow.at[t], r_yrow.at[t], q, mate)

    def pair_keys():
        return copy(keys.at[y], keys.at[y], s_ykey, r_ykey, q, mate)

    def stage_b(t):
        for k in range(1, R):
            row_copy(t, k).wait_recv()
        own_row_copy(t).wait()
        pair_copy(t).start()

    levels = lax.broadcasted_iota(jnp.int32, (span, B), 0)

    def partial_of(t, shard):
        acc = jnp.zeros((span, rows.shape[4]), f32)
        for side in range(PAIR):
            for r in range(R):
                hits = None
                for l in range(lookups):
                    key = keys[side, r, pl.ds(t * lookups + l, 1), :] - shard * span
                    hit = jnp.where(levels == key, 1.0, 0.0)
                    hits = hit if hits is None else hits + hit
                acc = acc + jnp.dot(hits.astype(bf16), rows[side, t, r], preferred_element_type=f32)
        return acc

    def up_copy(t, d):
        to = ((z + 1) % Z) * PAIR + y
        return copy(part.at[t, d], prcv.at[t, d + 1], s_part.at[t, d], r_part.at[t, d + 1], q, to)

    def down_copy(t, d):
        to = ((z + Z - 1) % Z) * PAIR + y
        return copy(part.at[t, d], prcv.at[t, d], s_part.at[t, d], r_part.at[t, d], q, to)

    def stage_c(t):
        pair_copy(t).wait_recv()

        def up(d):
            part[t, d] = partial_of(t, d * PAIR + y).astype(bf16)
            pl.when(z == 0)(lambda: up_copy(t, d).start())

        def down(d):
            part[t, d] = partial_of(t, d * PAIR + y).astype(bf16)
            pl.when(z == Z - 1)(lambda: down_copy(t, d).start())

        each(z + 1, Z, up)
        each(0, z, down)
        own[t] = partial_of(t, s)

    def stage_pass(t):
        def up(d):
            up_copy(t, d).wait_recv()
            part[t, d] = (part[t, d].astype(f32) + prcv[t, d + 1].astype(f32)).astype(bf16)
            up_copy(t, d).start()

        def down(d):
            down_copy(t, d).wait_recv()
            part[t, d] = (part[t, d].astype(f32) + prcv[t, d].astype(f32)).astype(bf16)
            down_copy(t, d).start()

        pl.when(z > 0)(lambda: each(z + 1, Z, up))
        pl.when(z < Z - 1)(lambda: each(0, z, down))

    def fin_copy(t, k):
        to = twin if k == 0 else (q + CORES * k) % R
        return copy(tab_out.at[q, t], tab_out.at[q, t], s_fin.at[t, k], r_fin.at[t, k], to, s)

    def fin_forward(t, k):
        origin = (q + R - CORES * k) % R
        return copy(tab_out.at[origin, t], tab_out.at[origin, t], s_fwd.at[t, k - 1], r_fwd.at[t, k - 1], twin, s)

    def stage_d(t):
        def from_below():
            up_copy(t, z).wait_recv()
            own[t] = own[t] + prcv[t, z + 1].astype(f32)

        def from_above():
            down_copy(t, z).wait_recv()
            own[t] = own[t] + prcv[t, z].astype(f32)

        pl.when(z > 0)(from_below)
        pl.when(z < Z - 1)(from_above)
        tab_out[q, t] = own[t].astype(bf16)
        for k in reversed(range(X)):
            fin_copy(t, k).start()

    def stage_e(t):
        for k in range(1, X):
            fin_copy(t, k).wait_recv()
            fin_forward(t, k).start()

    def t2_copy(k):
        to = (s + k) % S
        return copy(tsum.at[to], tred.at[k - 1], s_t2.at[k - 1], r_t2.at[k - 1], q, to)

    def t3_copy(k):
        to = (s + k) % S
        return copy(tfin, top_out.at[q, s], s_t3.at[k - 1], r_t3.at[k - 1], q, to)

    def t4_copy(k):
        to = twin if k == 0 else (q + CORES * k) % R
        return copy(top_out.at[q], top_out.at[q], s_t4.at[k], r_t4.at[k], to, s)

    def t5_copy(k):
        origin = (q + R - CORES * k) % R
        return copy(top_out.at[origin], top_out.at[origin], s_t5.at[k - 1], r_t5.at[k - 1], twin, s)

    def top_a():
        total = top_in[q].astype(f32)
        for k in range(1, R):
            top_copy(k).wait_recv()
            total = total + trcv[k - 1].astype(f32)
        tsum[...] = total.astype(bf16)
        each(1, S, lambda k: t2_copy(k).start())

    def top_b():
        each(1, S, lambda k: t2_copy(k).wait_recv())
        tfin[...] = lax.fori_loop(
            1, S, lambda k, a: a + tred[k - 1].astype(f32), tsum[s].astype(f32)
        ).astype(bf16)
        top_out[q, s] = tfin[...]
        each(1, S, lambda k: t3_copy(k).start())

    def top_c():
        each(1, S, lambda k: t3_copy(k).wait_recv())
        for k in reversed(range(X)):
            t4_copy(k).start()

    def top_d():
        for k in range(1, X):
            t4_copy(k).wait_recv()
            t5_copy(k).start()

    own_keys.wait()
    for k in range(1, R):
        key_copy(k).wait_recv()
    pair_keys().start()
    for t in range(min(2, T)):
        stage_b(t)
    pair_keys().wait_recv()

    def step(i, _):
        pl.when(i + 2 < T)(lambda: stage_b(i + 2))
        pl.when(i < T)(lambda: stage_c(i))
        for at, f in ((2, top_a), (4, top_b), (5, top_c), (7, top_d)):
            pl.when(i == at)(f)
        pl.when((i >= 1) & (i < T + 1))(lambda: stage_pass(i - 1))
        pl.when((i >= 3) & (i < T + 3))(lambda: stage_d(i - 3))
        pl.when((i >= 4) & (i < T + 4))(lambda: stage_e(i - 4))
        return 0

    lax.fori_loop(0, max(T + 4, 8), step, 0)

    def drain(t):
        for k in range(1, R):
            row_copy(t, k).wait_send()
        pair_copy(t).wait_send()
        each(z + 1, Z, lambda d: up_copy(t, d).wait_send())
        each(0, z, lambda d: down_copy(t, d).wait_send())
        fin_copy(t, 0).wait()
        for k in range(1, X):
            fin_copy(t, k).wait_send()
            fin_forward(t, k).wait()

    each(0, T, drain)
    for k in range(1, R):
        key_copy(k).wait_send()
        top_copy(k).wait_send()
    pair_keys().wait_send()
    each(1, S, lambda k: t2_copy(k).wait_send())
    each(1, S, lambda k: t3_copy(k).wait_send())
    t4_copy(0).wait()
    for k in range(1, X):
        t4_copy(k).wait_send()
        t5_copy(k).wait()


def finish_kernel(table_in, top_in, table_out, top_out, bias_out):
    def table(t, _):
        table_out[t] = table_in[t].astype(f32)
        return 0

    lax.fori_loop(0, table_out.shape[0], table, 0)
    features, width = top_out.shape[0], top_in.shape[2]
    for r in range(top_in.shape[0]):
        block = top_in[r, pl.ds(0, cdiv(features + 1, 16) * 16), :].astype(f32)
        top_out[:, pl.ds(r * width, width)] = block[:features]
        bias_out[:, pl.ds(r * width, width)] = block[features : features + 1]


def on_device(span, R, S, dense_out, pooled, top_weight, top_cotangent, indices):
    samples, emb = dense_out.shape
    tables, lookups = pooled.shape[1], indices.shape[2]
    nv = tables + 1
    features, hidden = top_weight.shape
    T = cdiv(tables, R)
    chunk_rows = cdiv(features + 1, 16 * S) * 16
    height = chunk_rows * S
    width = hidden // R
    pad_v = cdiv(nv, 8) * 8
    dense_grad, rows, top = pl.pallas_call(
        functools.partial(local_kernel, nv, 9, 32),
        out_shape=(
            jax.ShapeDtypeStruct((samples, emb), bf16),
            jax.ShapeDtypeStruct((R * T, samples, emb), bf16),
            jax.ShapeDtypeStruct((R, height, width), bf16),
        ),
        in_specs=[VMEM] * 4,
        out_specs=(VMEM,) * 3,
        scratch_shapes=[
            pltpu.VMEM((nv, emb, samples), f32),
            pltpu.VMEM((nv, pad_v, samples), f32),
            pltpu.VMEM((nv, pad_v, samples), f32),
            pltpu.VMEM((height, samples), f32),
            pltpu.VMEM((cdiv(features, 8) * 8, samples), f32),
            pltpu.VMEM((nv, emb, samples), f32),
        ],
        compiler_params=pltpu.CompilerParams(vmem_limit_bytes=48 << 20),
        name="local_math",
    )(dense_out, jnp.transpose(pooled, (1, 0, 2)), top_weight, top_cotangent)

    keys = jnp.transpose(indices, (1, 2, 0))
    keys = jnp.pad(keys, ((0, R * T - tables), (0, 0), (0, 0)), constant_values=-1)
    keys = keys.reshape(R, T * lookups, samples)
    key_rows = cdiv(T * lookups, 8) * 8
    keys = jnp.pad(keys, ((0, 0), (0, key_rows - T * lookups), (0, 0)), constant_values=-1)

    Z, X = S // PAIR, R // CORES
    dma = pltpu.SemaphoreType.DMA
    table_all, top_all = pl.pallas_call(
        functools.partial(comm_kernel, R, S, lookups),
        out_shape=(
            jax.ShapeDtypeStruct((R, T, span, emb), bf16),
            jax.ShapeDtypeStruct((R, S, chunk_rows, width), bf16),
        ),
        in_specs=[VMEM] * 3,
        out_specs=(VMEM,) * 2,
        scratch_shapes=[
            pltpu.VMEM((PAIR, T, R, samples, emb), bf16),
            pltpu.VMEM((PAIR, R, key_rows, samples), jnp.int32),
            pltpu.VMEM((T, Z, span, emb), bf16),
            pltpu.VMEM((T, Z + 1, span, emb), bf16),
            pltpu.VMEM((T, span, emb), f32),
            pltpu.VMEM((R - 1, S, chunk_rows, width), bf16),
            pltpu.VMEM((S, chunk_rows, width), bf16),
            pltpu.VMEM((S - 1, chunk_rows, width), bf16),
            pltpu.VMEM((chunk_rows, width), bf16),
            *[dma((T, R - 1))] * 2, *[dma((R - 1,))] * 4, *[dma((T,))] * 2, dma, dma,
            dma((T, Z)), dma((T, Z + 1)), *[dma((T, X))] * 2, *[dma((T, X - 1))] * 2,
            *[dma((S - 1,))] * 4, *[dma((X,))] * 2, *[dma((X - 1,))] * 2, dma((T,)), dma,
        ],
        compiler_params=pltpu.CompilerParams(
            collective_id=0, has_side_effects=True, vmem_limit_bytes=60 << 20
        ),
        name="exchange",
    )(rows.reshape(R, T, samples, emb), keys, top.reshape(R, S, chunk_rows, width))
    table_grad, top_grad, bias = pl.pallas_call(
        finish_kernel,
        out_shape=(
            jax.ShapeDtypeStruct((tables, span, emb), f32),
            jax.ShapeDtypeStruct((features, hidden), f32),
            jax.ShapeDtypeStruct((1, hidden), f32),
        ),
        in_specs=[VMEM] * 2,
        out_specs=(VMEM,) * 3,
        compiler_params=pltpu.CompilerParams(vmem_limit_bytes=48 << 20),
        name="finish",
    )(table_all.reshape(R * T, span, emb), top_all.reshape(R, height, width))
    bias_grad = bias.reshape(hidden)
    return dense_grad, top_grad, bias_grad, table_grad


ROWS_PER_SHARD = 256


def solution(mesh):
    return jax.shard_map(
        functools.partial(on_device, ROWS_PER_SHARD, mesh.shape["rep"], mesh.shape["shard"]),
        mesh=mesh,
        in_specs=(
            P(("rep", "shard"), None),
            P(("rep", "shard"), None, None),
            P(),
            P(("rep", "shard"), None),
            P(("rep", "shard"), None, None),
        ),
        out_specs=(P(("rep", "shard"), None), P(), P(), P(None, "shard", None)),
        check_vma=False,
    )
```
